512 devices in a mesh: group: 4 (over z_hi, core), gx: 32 (over z_lo, y), gy: 4 (over x).
Axes of the slice: x: 4, y: 4, z: 16 (z_hi: 2, z_lo: 8; z = z_hi * 8 + z_lo), core: 2. Of those that a mesh axis runs over, the one named last changes fastest.
Arguments:
- parent_mass: float32 [512, 512, 512], P('gx', ('group', 'gy')), may hold values from -6 to 6
- fine_mass: float32 [512, 128, 128], P('gx', ('group', 'gy')), may hold values from -6 to 6
- offsets: int32 [3], replicated, may hold values from 0 to 511
Outputs:
- parent_potential: float32 [512, 512, 512], P('gx', ('group', 'gy'))
- fine_potential: float32 [512, 128, 128], P('gx', ('group', 'gy'))
The draws below stay inside these ranges and needn't reach their ends.
All inputs are finite; a program needn't handle non-finite values.
Results may differ from the reference program's by a relative error of at most 0.0003.
Values sent between devices are 32-bit elements; how exact they have to be, the bound alone decides.
No kernel may reach another device: no remote copies, remote signals or barrier semaphores. Data moves between devices by JAX's collectives and lax.ppermute only.
A program may use at most 128 MiB of HBM per device.

```python
import math
import jax
import jax.numpy as jnp
from jax import lax

NP = 512
FZ = 128
CYCLES = 2
LEVELS = 3
SWEEPS = 2
COARSE_SWEEPS = 4
FX = 512
FY = 128


def block_scale(key, extent, split, least, top_value):
    loudness = 1.0
    for axis_at, blocks in split:
        draws = jax.random.uniform(jax.random.fold_in(jax.random.fold_in(key, 6), axis_at), (blocks,), jnp.float32, least / len(split), top_value / len(split))
        loudness = loudness * jnp.repeat(jnp.exp(draws), extent[axis_at] // blocks).reshape((-1,) + (1,) * (len(extent) - 1 - axis_at))
    return loudness


def scatter_about(rng, extent, spread, reach, cuts=(), held_as=jnp.bfloat16):
    gain = block_scale(rng, extent, cuts, -0.22, 0.18) if cuts else 1.0
    values = jax.random.normal(rng, extent, jnp.float32) * spread * gain
    return jnp.minimum(jnp.maximum(values, -reach), reach).astype(held_as)


def setup_inputs(seed: int = 0) -> dict:
    keys = jax.random.split(jax.random.key(seed), 4)
    return {
        "parent_mass": scatter_about(keys[0], (NP, NP, NP), 1.0, 6.0, ((0, 32), (1, 16)), jnp.float32),
        "fine_mass": scatter_about(keys[1], (FX, FY, FZ), 1.0, 6.0, ((0, 32), (1, 16)), jnp.float32),
        "offsets": jax.random.randint(keys[2], (3,), 0, NP).astype(jnp.int32),
    }


OMEGA = 6.0 / 7.0


def eigen(length):
    wave = jnp.arange(length).astype(jnp.float32)
    sine = jnp.sin(wave * (math.pi / length))
    return 4.0 * sine * sine


def coarsen(block):
    a, b, c = block.shape
    return block.reshape(a // 2, 2, b // 2, 2, c // 2, 2).sum(axis=(1, 3, 5))


def refine(block):
    return jnp.repeat(jnp.repeat(jnp.repeat(block, 2, axis=0), 2, axis=1), 2, axis=2)


def operate(field, edge):
    if edge:
        padded = jnp.pad(field, 1, mode="edge")
    else:
        padded = jnp.pad(field, 1)
    beside = padded[2:, 1:-1, 1:-1] + padded[:-2, 1:-1, 1:-1]
    beside = beside + padded[1:-1, 2:, 1:-1] + padded[1:-1, :-2, 1:-1]
    beside = beside + padded[1:-1, 1:-1, 2:] + padded[1:-1, 1:-1, :-2]
    return 6.0 * field - beside


def smooth(corr, resid, sweeps):
    for turn in range(sweeps):
        if corr is None:
            corr = (OMEGA / 6.0) * resid
        else:
            corr = corr + (OMEGA / 6.0) * (resid - operate(corr, False))
    return corr


def cycle(corr, resid, level):
    if level == LEVELS - 1:
        return smooth(None, resid, COARSE_SWEEPS)
    corr = smooth(corr, resid, SWEEPS)
    lower = 0.5 * coarsen(resid - operate(corr, False))
    below = cycle(None, lower, level + 1)
    corr = corr + refine(below)
    return smooth(corr, resid, SWEEPS)


def reference(parent_mass, fine_mass, offsets):
    rest = coarsen(fine_mass)
    placed = lax.dynamic_update_slice(jnp.zeros((NP, NP, NP), jnp.float32), rest, (0, 0, 0))
    placed = jnp.roll(placed, (offsets[0], offsets[1], offsets[2]), axis=(0, 1, 2))
    source = parent_mass + placed
    values = eigen(NP)
    half = NP // 2 + 1
    lam = values[:, None, None] + values[None, :, None] + values[None, None, :half]
    inverse = jnp.where(lam > 0, 1.0 / jnp.where(lam > 0, lam, 1.0), 0.0)
    spectrum = jnp.fft.rfftn(source) * inverse
    potential = jnp.fft.irfftn(spectrum, s=(NP, NP, NP)).astype(jnp.float32)
    moved = jnp.roll(potential, (-offsets[0], -offsets[1], -offsets[2]), axis=(0, 1, 2))
    footprint = moved[:FX // 2, :FY // 2, :FZ // 2]
    start = refine(footprint)
    resid = 2.0 * fine_mass - operate(start, True)
    corr = None
    for turn in range(CYCLES):
        corr = cycle(corr, resid, 0)
    return potential, start + corr
```

```python
import math

import jax
import jax.numpy as jnp
import numpy as np
from jax import lax
from jax.experimental import pallas as pl
from jax.experimental.pallas import tpu as pltpu
from jax.sharding import PartitionSpec as P

NP = 512
CYCLES = 2
LEVELS = 3
SWEEPS = 2
COARSE_SWEEPS = 4

OMEGA = 6.0 / 7.0
F32 = jnp.float32
BF16 = jnp.bfloat16
ALL = ("group", "gy", "gx")
GX = 32
YY = 16
WX = NP // GX
WY = NP // YY
SX = 256
SY = 64
SZ = 64
HX = 4
HY = 6
LANES = 128
FORE = 5
BACK = 6


def split(x):
    high = x.astype(BF16)
    return high, (x - high.astype(F32)).astype(BF16)


def product(a, b, dims):
    def dot(u, v):
        return lax.dot_general(u, v, (dims, ((), ())), preferred_element_type=F32)

    return dot(a[0], b[0]) + (dot(a[0], b[1]) + dot(a[1], b[0]))


NN = ((1,), (0,))
NT = ((1,), (1,))


def forward_kernel(offsets, mass, fine, high, low, pairs, out, beside):
    for i in range(8):
        beside[8 * i : 8 * i + 8, :] = fine[2 * i] + fine[2 * i + 1]
    both = beside[pl.ds(0, 32, stride=2), :] + beside[pl.ds(1, 32, stride=2), :]
    first = both.astype(BF16)
    left = both - first.astype(F32)
    second = left.astype(BF16)
    third = (left - second.astype(F32)).astype(BF16)
    add = pairs[...]

    def dot(u):
        return lax.dot_general(u, add, (NN, ((), ())), preferred_element_type=F32)

    rest = dot(first) + (dot(second) + dot(third))
    rest = jnp.concatenate([rest, jnp.zeros((96, LANES), F32)], axis=0)
    rest = jnp.concatenate([rest, jnp.zeros((LANES, NP - LANES), F32)], axis=1)
    rest = pltpu.roll(rest, offsets[2], 1)
    table = (high[...], low[...])
    dense = product(table, split(mass[...]), NT)
    for c in range(4):
        out[pl.ds(c, NP, stride=FORE), :] = dense[:, c * LANES : (c + 1) * LANES]
    out[pl.ds(4, NP, stride=FORE), :] = product(table, split(rest), NT)


def place(group, amount, shift, total, value):
    amount = amount % LANES
    if amount:
        value = pltpu.roll(value, amount, 1)
    if total is None:
        return value
    return jnp.where(group == shift, value, total)


def plane_kernel(offsets, wave, got, high, low, column, row, out, plane0, plane1, plane2, plane3, rest):
    plane = (plane0, plane1, plane2, plane3)
    lane = lax.broadcasted_iota(jnp.int32, (GX, LANES), 1)
    group = lane // WY
    for a in range(4):
        for b in range(4):
            parts = [got[pl.ds((b * 4 + q) * GX * FORE + a, GX, stride=FORE), :] for q in range(4)]
            for p in range(4):
                total = None
                for q in range(4):
                    total = place(group, (q - p) * WY, q, total, parts[q])
                plane[b][pl.ds(a * 4 + p, GX, stride=WX), :] = total
    light = lane // 4
    parts = [got[pl.ds(q * GX * FORE + 4, GX, stride=FORE), :] for q in range(YY)]
    for p in range(8):
        total = jnp.zeros((GX, LANES), F32)
        for q in range(YY):
            total = place(light, (q - p) * 4, q, total, parts[q])
        rest[pl.ds(p, GX, stride=8), :] = total
    wide = jnp.concatenate([rest[0:SX, :], jnp.zeros((SX, NP - LANES), F32)], axis=1)
    wide = pltpu.roll(wide, offsets[1], 1)
    wide = jnp.concatenate([wide, jnp.zeros((NP - SX, NP), F32)], axis=0)
    wide = pltpu.roll(wide, offsets[0], 0)
    table = (high[...], low[...])
    half = product(table, split(jnp.concatenate([part[...] for part in plane], axis=1) + wide), NN)
    spectrum = product(split(half), table, NN)
    lam = column[...] + (row[...] + wave[0])
    spectrum = spectrum * jnp.where(lam > 0, (1.0 / float(NP**3)) / jnp.where(lam > 0, lam, 1.0), 0.0)
    half = product(split(spectrum), table, NN)
    whole = product(table, split(half), NN)
    for b in range(4):
        plane[b][...] = whole[:, b * LANES : (b + 1) * LANES]
    near = pltpu.roll(whole, (NP - offsets[0]) % NP, 0)[0:SX, :]
    near = pltpu.roll(near, (NP + HY - offsets[1]) % NP, 1)[:, 0:LANES]
    place_of = lax.broadcasted_iota(jnp.int32, (SX, LANES), 1)
    near = jnp.where(place_of < HY, near[:, HY : HY + 1], near)
    near = jnp.where(place_of >= HY + SY, near[:, HY + SY - 1 : HY + SY], near)
    rest[HX : HX + SX, :] = near
    rest[0:HX, :] = jnp.broadcast_to(near[0:1, :], (HX, LANES))
    rest[HX + SX : 2 * HX + SX, :] = jnp.broadcast_to(near[SX - 1 : SX, :], (HX, LANES))
    for a in range(4):
        for b in range(4):
            parts = [plane[b][pl.ds(a * 4 + p, GX, stride=WX), :] for p in range(4)]
            for q in range(4):
                total = None
                for p in range(4):
                    total = place(group, (p - q) * WY, p, total, parts[p])
                out[pl.ds((b * 4 + q) * GX * BACK + a, GX, stride=BACK), :] = total
    wing = lane // 16
    for h in range(2):
        parts = [rest[pl.ds(h * 8 + p, GX, stride=8), :] for p in range(8)]
        for q in range(YY):
            total = None
            for p in range(8):
                total = place(wing, p * 16 - 4 * q, p, total, parts[p])
            out[pl.ds(q * GX * BACK + 4 + h, GX, stride=BACK), :] = total


def near_kernel(offsets, got, high, low, out):
    table = (high[...], low[...])
    back = (NP - offsets[2]) % NP
    for h in range(2):
        turned = got[pl.ds(4 + h, NP, stride=BACK), :].T
        rows = product(split(turned), table, NN)
        out[h * LANES : (h + 1) * LANES, :] = pltpu.roll(rows, back, 1)[:, 0:LANES]


def whole_kernel(got, high, low, out):
    table = (high[...], low[...])
    for c in range(4):
        turned = got[pl.ds(c, NP, stride=BACK), :].T
        out[c * LANES : (c + 1) * LANES, :] = product(split(turned), table, NN)


def cas_tables():
    wave = np.arange(NP)
    angle = (wave[:, None] * wave[None, :] % NP) * (2.0 * np.pi / NP)
    return jnp.asarray((np.cos(angle) + np.sin(angle)).astype(np.float32))


def eigenvalues():
    sine = np.sin(np.arange(NP) * (np.pi / NP))
    return (4.0 * sine * sine).astype(np.float32)


VMEM = pl.BlockSpec(memory_space=pltpu.VMEM)
SMEM = pl.BlockSpec(memory_space=pltpu.SMEM)
PARAMS = pltpu.CompilerParams(vmem_limit_bytes=56 * 1024 * 1024)
INTERPRET = False


def call(body, name, ins, shape, scratch=()):
    return pl.pallas_call(
        body,
        name=name,
        in_specs=ins,
        out_specs=VMEM,
        out_shape=jax.ShapeDtypeStruct(shape, F32),
        scratch_shapes=list(scratch),
        compiler_params=PARAMS,
        interpret=INTERPRET,
    )


def forward(offsets, mass, fine, high, low, pairs):
    return call(forward_kernel, "forward", [SMEM] + [VMEM] * 5, (NP * FORE, LANES), [pltpu.VMEM((64, LANES), F32)])(
        offsets, mass, fine, high, low, pairs
    )


def spectral(offsets, wave, got, high, low, column, row):
    return call(
        plane_kernel,
        "plane",
        [SMEM, SMEM] + [VMEM] * 5,
        (NP * BACK, LANES),
        [pltpu.VMEM((NP, LANES), F32)] * 4 + [pltpu.VMEM((SX + 8, LANES), F32)],
    )(offsets, wave, got, high, low, column, row)


def near_back(offsets, got, high, low):
    return call(near_kernel, "near", [SMEM] + [VMEM] * 3, (256, LANES))(offsets, got, high, low)


def whole_back(got, high, low):
    return call(whole_kernel, "whole", [VMEM] * 3, (NP, NP))(got, high, low)


def swap(piece, lanes):
    piece = piece.reshape(NP, 1, lanes)
    return lax.all_to_all(piece, ALL, 0, 0, tiled=True).reshape(NP * lanes // LANES, LANES)


def constants():
    high, low = split(cas_tables())
    pairs = np.zeros((LANES, LANES), np.float32)
    pairs[np.arange(LANES), np.arange(LANES) // 2] = 1.0
    eigen = eigenvalues()
    return high, low, jnp.asarray(pairs, BF16), jnp.asarray(eigen[:, None]), jnp.asarray(eigen[None, :]), jnp.asarray(eigen)


XF = 32
YF = 24
X1 = 40
Y1 = 64
X2 = 20
Y2 = 32
STEP = 1.0 / 7.0


def exact(value, table):
    first = value.astype(BF16)
    left = value - first.astype(F32)
    second = left.astype(BF16)
    third = (left - second.astype(F32)).astype(BF16)

    def dot(u):
        return lax.dot_general(u, table, (NN, ((), ())), preferred_element_type=F32)

    return dot(first) + (dot(second) + dot(third))


def over(count, body, per=4):
    def group(t, carry):
        for k in range(per):
            body(t * per + k)
        return carry

    lax.fori_loop(0, count // per, group, 0)


def lanes_of(rows):
    return lax.broadcasted_iota(jnp.int32, (rows, LANES), 1)


def rows_of(rows):
    return lax.broadcasted_iota(jnp.int32, (rows, LANES), 0)


def inside(place, count):
    return jnp.where((place >= 0) & (place < count), 1.0, 0.0).astype(F32)


class Fine:
    def __init__(self, pos):
        self.first = 16 * pos[0] - 8
        self.count = 512
        self.x = XF
        y = rows_of(YF) + (8 * pos[1] - 8)
        self.mask = jnp.where((y >= 0) & (y < 128), STEP, 0.0)
        lane = lanes_of(YF)
        self.low = jnp.where(lane == 0, 0.0, 1.0)
        self.high = jnp.where(lane == LANES - 1, 0.0, 1.0)

    def around(self, ref, x):
        c = ref[x + 1]
        near = ref[x] + ref[x + 2]
        near = near + (pltpu.roll(c, 1, 0) + pltpu.roll(c, YF - 1, 0))
        near = near + (pltpu.roll(c, 1, 1) * self.low + pltpu.roll(c, LANES - 1, 1) * self.high)
        return c, near


class Coarse:
    def __init__(self, first, count, x, y, z):
        self.first = first
        self.count = count
        self.x = x
        self.y = y
        self.mask = jnp.where(lanes_of(y) < z, STEP, 0.0)
        row = rows_of(y)
        self.low = jnp.where(row == 0, 0.0, 1.0)
        self.high = jnp.where(row == y - 1, 0.0, 1.0)

    def around(self, ref, x):
        c = ref[x + 1]
        near = ref[x] + ref[x + 2]
        near = near + (pltpu.roll(c, 1, 0) * self.low + pltpu.roll(c, self.y - 1, 0) * self.high)
        near = near + (pltpu.roll(c, 1, 1) + pltpu.roll(c, LANES - 1, 1))
        return c, near


def sweep(level, source, right, shift, target):
    def body(x):
        c, near = level.around(source, x)
        scale = inside(level.first + x, level.count)
        target[x + 1] = (right[x + shift] + (c + near)) * (level.mask * scale)

    over(level.x, body)


def clear(ref, size):
    ref[0] = jnp.zeros(ref.shape[1:], F32)
    ref[size + 1] = jnp.zeros(ref.shape[1:], F32)


def lower_of(level, corr, resid, strip, pairs, out):
    def left(x):
        c, near = level.around(corr, x)
        return (resid[x] - (6.0 * c - near))[8:16]

    for k in range(8):
        strip[8 * k : 8 * k + 8, :] = left(8 + 2 * k) + left(9 + 2 * k)
    both = strip[pl.ds(0, 32, stride=2), :] + strip[pl.ds(1, 32, stride=2), :]
    small = 0.5 * exact(both, pairs)
    out[...] = small[0:16] + pltpu.roll(small[16:32], 64, 1)


def open_kernel(pos, near, fine, pairs, spread, start, resid, corr, lower, wide, first, second, tall, twice, strip):
    level = Fine(pos)
    tall[...] = exact(near[...], spread[...])
    for i in range(16):
        value = tall[i * 16 + 2 : i * 16 + 14, :]
        twice[pl.ds(0, 12, stride=2), :] = value
        twice[pl.ds(1, 12, stride=2), :] = value
        wide[1 + 2 * i] = twice[...]
        wide[2 + 2 * i] = twice[...]
    clear(wide, XF)
    clear(first, XF)
    clear(second, XF)
    for k in range(16):
        start[k] = wide[9 + k][8:16]

    def body(x):
        c, around = level.around(wide, x)
        edge = c * ((1.0 - level.low) + (1.0 - level.high))
        value = 2.0 * fine[x] - (6.0 * c - (around + edge))
        scale = inside(level.first + x, level.count)
        held = jnp.where(level.mask * scale > 0.0, value, 0.0)
        resid[x] = held
        first[x + 1] = held * STEP

    over(XF, body)
    sweep(level, first, resid, 0, second)
    corr[...] = second[1 : XF + 1]
    lower_of(level, second, resid, strip, pairs[...], lower)


def coarse(pos, blocks, corr, resid, pairs, spread, one, scratch):
    right1, left1, other1, right2, left2, other2, rows, double, grown, twice, first, second = scratch
    level1 = Coarse(8 * pos[0] - 16, 256, X1, Y1, 64)
    level2 = Coarse(4 * pos[0] - 8, 128, X2, Y2, 32)
    fine = Fine(pos)
    lane = lanes_of(Y1)
    for ref in (left1, other1):
        clear(ref, X1)
    for ref in (left2, other2):
        clear(ref, X2)
    for b, block in enumerate(blocks):
        for xx in range(4):
            value = block[xx]
            for half in range(2):
                held = jnp.where(lane < 64, pltpu.roll(value, 64, 1) if half else value, 0.0)
                right1[b * 8 + half * 4 + xx] = held
                left1[1 + b * 8 + half * 4 + xx] = held * STEP
    sweep(level1, left1, right1, 0, other1)

    def down(k):
        total = None
        for a in range(2):
            c, near = level1.around(other1, 2 * k + a)
            value = right1[2 * k + a] - (6.0 * c - near)
            total = value if total is None else total + value
        double[...] = total
        rows[pl.ds(pl.multiple_of(k * Y2, Y2), Y2), :] = double[pl.ds(0, Y2, stride=2), :] + double[pl.ds(1, Y2, stride=2), :]

    over(X2, down, 1)
    rows[...] = exact(rows[...], pairs)

    def begin(k):
        value = rows[pl.ds(pl.multiple_of(k * Y2, Y2), Y2), :]
        scale = inside(level2.first + k, level2.count)
        value = jnp.where(level2.mask * scale > 0.0, 0.5 * value, 0.0)
        right2[k] = value
        left2[k + 1] = value * STEP

    over(X2, begin)
    sweep(level2, left2, right2, 0, other2)
    sweep(level2, other2, right2, 0, left2)
    sweep(level2, left2, right2, 0, other2)
    rows[...] = exact(other2[1 : X2 + 1].reshape(X2 * Y2, LANES), spread)

    def up(k):
        value = rows[pl.ds(pl.multiple_of(k * Y2, Y2), Y2), :]
        double[pl.ds(0, Y2, stride=2), :] = value
        double[pl.ds(1, Y2, stride=2), :] = value
        value = double[...]
        other1[1 + 2 * k] = other1[1 + 2 * k] + value
        other1[2 + 2 * k] = other1[2 + 2 * k] + value

    over(X2, up, 1)
    sweep(level1, other1, right1, 0, left1)
    sweep(level1, left1, right1, 0, other1)
    amount = 124 - 4 * pos[1]
    for k in range(16):
        value = other1[13 + k]
        value = jnp.concatenate([jnp.zeros((8, LANES), F32), value, jnp.zeros((56, LANES), F32)], axis=0)
        grown[k * 16 : k * 16 + 16, :] = pltpu.roll(value, amount, 0)[0:16]
    grown[...] = exact(grown[...], spread)
    clear(first, XF)
    clear(second, XF)
    for i in range(16):
        value = grown[i * 16 : i * 16 + 12, :]
        twice[pl.ds(0, 12, stride=2), :] = value
        twice[pl.ds(1, 12, stride=2), :] = value
        first[1 + 2 * i] = corr[2 * i] + twice[...]
        first[2 + 2 * i] = corr[2 * i + 1] + twice[...]
    sweep(fine, first, resid, 0, second)
    sweep(fine, second, resid, 0, first)
    return fine


def turn_kernel(pos, b0, b1, b2, b3, b4, corr, resid, pairs, spread, after, lower, *scratch):
    strip, scratch = scratch[-1], scratch[:-1]
    fine = coarse(pos, (b0, b1, b2, b3, b4), corr, resid, pairs[...], spread[...], None, scratch)
    first, second = scratch[-2:]
    sweep(fine, first, resid, 0, second)
    sweep(fine, second, resid, 0, first)
    after[...] = first[1 : XF + 1]
    lower_of(fine, first, resid, strip, pairs[...], lower)


def close_kernel(pos, b0, b1, b2, b3, b4, corr, resid, pairs, spread, start, out, *scratch):
    coarse(pos, (b0, b1, b2, b3, b4), corr, resid, pairs[...], spread[...], None, scratch)
    first = scratch[-2]
    for k in range(16):
        out[k] = start[k] + first[9 + k][8:16]


def held(*shape):
    return pltpu.VMEM(shape, F32)


def shaped(*shape):
    return jax.ShapeDtypeStruct(shape, F32)


def inner():
    return [
        held(X1, Y1, LANES),
        held(X1 + 2, Y1, LANES),
        held(X1 + 2, Y1, LANES),
        held(X2, Y2, LANES),
        held(X2 + 2, Y2, LANES),
        held(X2 + 2, Y2, LANES),
        held(X2 * Y2, LANES),
        held(Y1, LANES),
        held(256, LANES),
        held(YF, LANES),
        held(XF + 2, YF, LANES),
        held(XF + 2, YF, LANES),
    ]


def many(body, name, count, shapes, scratch):
    return pl.pallas_call(
        body,
        name=name,
        in_specs=[SMEM] + [VMEM] * count,
        out_specs=[VMEM] * len(shapes),
        out_shape=shapes,
        scratch_shapes=scratch,
        compiler_params=PARAMS,
        interpret=INTERPRET,
    )


def opening(pos, near, fine, pairs, spread):
    shapes = [shaped(16, 8, LANES), shaped(XF, YF, LANES), shaped(XF, YF, LANES), shaped(16, LANES)]
    scratch = [held(XF + 2, YF, LANES)] * 3 + [held(256, LANES), held(YF, LANES), held(64, LANES)]
    return many(open_kernel, "opening", 4, shapes, scratch)(pos, near, fine, pairs, spread)


def turning(pos, blocks, corr, resid, pairs, spread):
    shapes = [shaped(XF, YF, LANES), shaped(16, LANES)]
    return many(turn_kernel, "turning", 9, shapes, inner() + [held(64, LANES)])(pos, *blocks, corr, resid, pairs, spread)


def closing(pos, blocks, corr, resid, pairs, spread, start):
    return many(close_kernel, "closing", 10, [shaped(16, 8, LANES)], inner())(
        pos, *blocks, corr, resid, pairs, spread, start
    )[0]


def shifted(value, axes, size, step):
    return lax.ppermute(value, axes, [(i, i + step) for i in range(size) if 0 <= i + step < size])


def gather(lower):
    every = jnp.broadcast_to(lower[None], (YY, 16, LANES))
    every = lax.all_to_all(every, ("group", "gy"), 0, 0, tiled=True)
    block = every.reshape(YY, 4, 4, LANES).transpose(1, 0, 2, 3).reshape(4, Y1, LANES)
    return [block if step == 0 else shifted(block, "gx", GX, step) for step in (2, 1, 0, -1, -2)]


def widened(fine):
    sides = ("group", "gy")
    tall = jnp.concatenate([shifted(fine, sides, YY, 1), fine, shifted(fine, sides, YY, -1)], axis=1)
    before = shifted(tall[8:16], "gx", GX, 1)
    behind = shifted(tall[0:8], "gx", GX, -1)
    return jnp.concatenate([before, tall, behind], axis=0)


def local(parent_mass, fine_mass, offsets):
    high, low, pairs, column, row, eigen = constants()
    spread = pairs.T
    pos = jnp.stack([lax.axis_index("gx"), lax.axis_index(("group", "gy"))]).astype(jnp.int32)
    wave = lax.dynamic_slice(eigen, (lax.axis_index(ALL),), (1,))
    wide = widened(fine_mass)
    got = swap(forward(offsets, parent_mass.reshape(NP, NP), fine_mass, high, low, pairs), FORE * LANES)
    got = swap(spectral(offsets, wave, got, high, low, column, row), BACK * LANES)
    near = near_back(offsets, got, high, low)
    start, resid, corr, lower = opening(pos, near, wide, pairs, spread)
    potential = whole_back(got, high, low)
    corr, lower = turning(pos, gather(lower), corr, resid, pairs, spread)
    out = closing(pos, gather(lower), corr, resid, pairs, spread, start)
    return (potential.reshape(WX, WY, NP), out)


def solution(mesh):
    spec = P("gx", ("group", "gy"), None)
    return jax.shard_map(
        local,
        mesh=mesh,
        in_specs=(spec, spec, P()),
        out_specs=(spec, spec),
        check_vma=False,
    )
```

```python
import math

import jax
import jax.numpy as jnp
import numpy as np
from jax import lax
from jax.experimental import pallas as pl
from jax.experimental.pallas import tpu as pltpu
from jax.sharding import PartitionSpec as P

NP = 512
CYCLES = 2
LEVELS = 3
SWEEPS = 2
COARSE_SWEEPS = 4

OMEGA = 6.0 / 7.0
F32 = jnp.float32
BF16 = jnp.bfloat16
ALL = ("group", "gy", "gx")
GX = 32
YY = 16
WX = NP // GX
WY = NP // YY
SX = 256
SY = 64
SZ = 64
HX = 4
HY = 6
LANES = 128
FORE = 5
BACK = 6


def split(x):
    high = x.astype(BF16)
    return high, (x - high.astype(F32)).astype(BF16)


def product(a, b, dims):
    def dot(u, v):
        return lax.dot_general(u, v, (dims, ((), ())), preferred_element_type=F32)

    return dot(a[0], b[0]) + (dot(a[0], b[1]) + dot(a[1], b[0]))


NN = ((1,), (0,))
NT = ((1,), (1,))


def forward_kernel(offsets, mass, fine, high, low, pairs, out, beside):
    for i in range(8):
        beside[8 * i : 8 * i + 8, :] = fine[2 * i] + fine[2 * i + 1]
    both = beside[pl.ds(0, 32, stride=2), :] + beside[pl.ds(1, 32, stride=2), :]
    first = both.astype(BF16)
    left = both - first.astype(F32)
    second = left.astype(BF16)
    third = (left - second.astype(F32)).astype(BF16)
    add = pairs[...]

    def dot(u):
        return lax.dot_general(u, add, (NN, ((), ())), preferred_element_type=F32)

    rest = dot(first) + (dot(second) + dot(third))
    rest = jnp.concatenate([rest, jnp.zeros((96, LANES), F32)], axis=0)
    rest = jnp.concatenate([rest, jnp.zeros((LANES, NP - LANES), F32)], axis=1)
    rest = pltpu.roll(rest, offsets[2], 1)
    table = (high[...], low[...])
    dense = product(table, split(mass[...]), NT)
    for c in range(4):
        out[pl.ds(c, NP, stride=FORE), :] = dense[:, c * LANES : (c + 1) * LANES]
    out[pl.ds(4, NP, stride=FORE), :] = product(table, split(rest), NT)


def place(group, amount, shift, total, value):
    amount = amount % LANES
    if amount:
        value = pltpu.roll(value, amount, 1)
    if total is None:
        return value
    return jnp.where(group == shift, value, total)


def plane_kernel(offsets, wave, got, high, low, column, row, out, plane0, plane1, plane2, plane3, rest):
    plane = (plane0, plane1, plane2, plane3)
    lane = lax.broadcasted_iota(jnp.int32, (GX, LANES), 1)
    group = lane // WY
    for a in range(4):
        for b in range(4):
            parts = [got[pl.ds((b * 4 + q) * GX * FORE + a, GX, stride=FORE), :] for q in range(4)]
            for p in range(4):
                total = None
                for q in range(4):
                    total = place(group, (q - p) * WY, q, total, parts[q])
                plane[b][pl.ds(a * 4 + p, GX, stride=WX), :] = total
    light = lane // 4
    parts = [got[pl.ds(q * GX * FORE + 4, GX, stride=FORE), :] for q in range(YY)]
    for p in range(8):
        total = jnp.zeros((GX, LANES), F32)
        for q in range(YY):
            total = place(light, (q - p) * 4, q, total, parts[q])
        rest[pl.ds(p, GX, stride=8), :] = total
    wide = jnp.concatenate([rest[0:SX, :], jnp.zeros((SX, NP - LANES), F32)], axis=1)
    wide = pltpu.roll(wide, offsets[1], 1)
    wide = jnp.concatenate([wide, jnp.zeros((NP - SX, NP), F32)], axis=0)
    wide = pltpu.roll(wide, offsets[0], 0)
    table = (high[...], low[...])
    half = product(table, split(jnp.concatenate([part[...] for part in plane], axis=1) + wide), NN)
    spectrum = product(split(half), table, NN)
    lam = column[...] + (row[...] + wave[0])
    spectrum = spectrum * jnp.where(lam > 0, (1.0 / float(NP**3)) / jnp.where(lam > 0, lam, 1.0), 0.0)
    half = product(split(spectrum), table, NN)
    whole = product(table, split(half), NN)
    for b in range(4):
        plane[b][...] = whole[:, b * LANES : (b + 1) * LANES]
    near = pltpu.roll(whole, (NP - offsets[0]) % NP, 0)[0:SX, :]
    near = pltpu.roll(near, (NP + HY - offsets[1]) % NP, 1)[:, 0:LANES]
    place_of = lax.broadcasted_iota(jnp.int32, (SX, LANES), 1)
    near = jnp.where(place_of < HY, near[:, HY : HY + 1], near)
    near = jnp.where(place_of >= HY + SY, near[:, HY + SY - 1 : HY + SY], near)
    rest[HX : HX + SX, :] = near
    rest[0:HX, :] = jnp.broadcast_to(near[0:1, :], (HX, LANES))
    rest[HX + SX : 2 * HX + SX, :] = jnp.broadcast_to(near[SX - 1 : SX, :], (HX, LANES))
    for a in range(4):
        for b in range(4):
            parts = [plane[b][pl.ds(a * 4 + p, GX, stride=WX), :] for p in range(4)]
            for q in range(4):
                total = None
                for p in range(4):
                    total = place(group, (p - q) * WY, p, total, parts[p])
                out[pl.ds((b * 4 + q) * GX * BACK + a, GX, stride=BACK), :] = total
    wing = lane // 16
    for h in range(2):
        parts = [rest[pl.ds(h * 8 + p, GX, stride=8), :] for p in range(8)]
        for q in range(YY):
            total = None
            for p in range(8):
                total = place(wing, p * 16 - 4 * q, p, total, parts[p])
            out[pl.ds(q * GX * BACK + 4 + h, GX, stride=BACK), :] = total


def near_kernel(offsets, got, high, low, out):
    table = (high[...], low[...])
    back = (NP - offsets[2]) % NP
    for h in range(2):
        turned = got[pl.ds(4 + h, NP, stride=BACK), :].T
        rows = product(split(turned), table, NN)
        out[h * LANES : (h + 1) * LANES, :] = pltpu.roll(rows, back, 1)[:, 0:LANES]


def whole_kernel(got, high, low, out):
    table = (high[...], low[...])
    for c in range(4):
        turned = got[pl.ds(c, NP, stride=BACK), :].T
        out[c * LANES : (c + 1) * LANES, :] = product(split(turned), table, NN)


def cas_tables():
    wave = np.arange(NP)
    angle = (wave[:, None] * wave[None, :] % NP) * (2.0 * np.pi / NP)
    return jnp.asarray((np.cos(angle) + np.sin(angle)).astype(np.float32))


def eigenvalues():
    sine = np.sin(np.arange(NP) * (np.pi / NP))
    return (4.0 * sine * sine).astype(np.float32)


VMEM = pl.BlockSpec(memory_space=pltpu.VMEM)
SMEM = pl.BlockSpec(memory_space=pltpu.SMEM)
PARAMS = pltpu.CompilerParams(vmem_limit_bytes=56 * 1024 * 1024)
INTERPRET = False


def call(body, name, ins, shape, scratch=()):
    return pl.pallas_call(
        body,
        name=name,
        in_specs=ins,
        out_specs=VMEM,
        out_shape=jax.ShapeDtypeStruct(shape, F32),
        scratch_shapes=list(scratch),
        compiler_params=PARAMS,
        interpret=INTERPRET,
    )


def forward(offsets, mass, fine, high, low, pairs):
    return call(forward_kernel, "forward", [SMEM] + [VMEM] * 5, (NP * FORE, LANES), [pltpu.VMEM((64, LANES), F32)])(
        offsets, mass, fine, high, low, pairs
    )


def spectral(offsets, wave, got, high, low, column, row):
    return call(
        plane_kernel,
        "plane",
        [SMEM, SMEM] + [VMEM] * 5,
        (NP * BACK, LANES),
        [pltpu.VMEM((NP, LANES), F32)] * 4 + [pltpu.VMEM((SX + 8, LANES), F32)],
    )(offsets, wave, got, high, low, column, row)


def near_back(offsets, got, high, low):
    return call(near_kernel, "near", [SMEM] + [VMEM] * 3, (256, LANES))(offsets, got, high, low)


def whole_back(got, high, low):
    return call(whole_kernel, "whole", [VMEM] * 3, (NP, NP))(got, high, low)


def swap(piece, lanes):
    piece = piece.reshape(NP, 1, lanes)
    return lax.all_to_all(piece, ALL, 0, 0, tiled=True).reshape(NP * lanes // LANES, LANES)


def constants():
    high, low = split(cas_tables())
    pairs = np.zeros((LANES, LANES), np.float32)
    pairs[np.arange(LANES), np.arange(LANES) // 2] = 1.0
    eigen = eigenvalues()
    return high, low, jnp.asarray(pairs, BF16), jnp.asarray(eigen[:, None]), jnp.asarray(eigen[None, :]), jnp.asarray(eigen)


XF = 32
YF = 24
X1 = 20
Y1 = 32
X2 = 10
Y2 = 16
HALF = 64
STEP = 1.0 / 7.0


def exact(value, table):
    first = value.astype(BF16)
    left = value - first.astype(F32)
    second = left.astype(BF16)
    third = (left - second.astype(F32)).astype(BF16)

    def dot(u):
        return lax.dot_general(u, table, (NN, ((), ())), preferred_element_type=F32)

    return dot(first) + (dot(second) + dot(third))


def over(count, body, per=4, base=0):
    def group(t, carry):
        for k in range(per):
            body(base + t * per + k)
        return carry

    lax.fori_loop(0, count // per, group, 0)


def lanes_of(rows):
    return lax.broadcasted_iota(jnp.int32, (rows, LANES), 1)


def rows_of(rows):
    return lax.broadcasted_iota(jnp.int32, (rows, LANES), 0)


def inside(place, count):
    return jnp.where((place >= 0) & (place < count), 1.0, 0.0).astype(F32)


class Fine:
    def __init__(self, pos):
        self.first = 16 * pos[0] - 8
        self.count = 512
        self.x = XF
        y = rows_of(YF) + (8 * pos[1] - 8)
        self.mask = jnp.where((y >= 0) & (y < 128), STEP, 0.0)
        lane = lanes_of(YF)
        self.low = jnp.where(lane == 0, 0.0, 1.0)
        self.high = jnp.where(lane == LANES - 1, 0.0, 1.0)

    def scale(self, x):
        return self.mask * inside(self.first + x, self.count)

    def around(self, ref, x):
        c = ref[x + 1]
        near = ref[x] + ref[x + 2]
        near = near + (pltpu.roll(c, 1, 0) + pltpu.roll(c, YF - 1, 0))
        near = near + (pltpu.roll(c, 1, 1) * self.low + pltpu.roll(c, LANES - 1, 1) * self.high)
        return c, near


class Coarse:
    def __init__(self, first, count, x, y, first_y, count_y, z):
        self.first = first
        self.count = count
        self.x = x
        row = rows_of(y) + first_y
        lane = lanes_of(y)
        self.y = y
        self.left = lane < HALF
        place = lane % HALF
        self.mask = jnp.where((place < z) & (row >= 0) & (row < count_y), STEP, 0.0)
        self.low = jnp.where(place == 0, 0.0, 1.0)
        self.high = jnp.where(place == HALF - 1, 0.0, 1.0)

    def scale(self, x):
        here = inside(self.first + x, self.count)
        there = inside(self.first + self.x + x, self.count)
        return self.mask * jnp.where(self.left, here, there)

    def around(self, ref, x):
        c = ref[x + 1]
        near = ref[x] + ref[x + 2]
        near = near + (pltpu.roll(c, 1, 0) + pltpu.roll(c, self.y - 1, 0))
        near = near + (pltpu.roll(c, 1, 1) * self.low + pltpu.roll(c, LANES - 1, 1) * self.high)
        return c, near

    def join(self, ref):
        ref[0] = jnp.where(self.left, 0.0, pltpu.roll(ref[self.x], HALF, 1))
        ref[self.x + 1] = jnp.where(self.left, pltpu.roll(ref[1], HALF, 1), 0.0)


def sweep(level, source, right, target, per=4, base=0, count=None):
    def body(x):
        c, near = level.around(source, x)
        target[x + 1] = (right[x] + (c + near)) * level.scale(x)

    over(level.x if count is None else count, body, per, base)


def clear(ref, size):
    ref[0] = jnp.zeros(ref.shape[1:], F32)
    ref[size + 1] = jnp.zeros(ref.shape[1:], F32)


def lower_of(level, corr, resid, strip, pairs, out):
    def left(x):
        c, near = level.around(corr, x)
        return (resid[x] - (6.0 * c - near))[8:16]

    for k in range(8):
        strip[8 * k : 8 * k + 8, :] = left(8 + 2 * k) + left(9 + 2 * k)
    both = strip[pl.ds(0, 32, stride=2), :] + strip[pl.ds(1, 32, stride=2), :]
    small = 0.5 * exact(both, pairs)
    out[...] = small[0:16] + pltpu.roll(small[16:32], 64, 1)


def open_kernel(pos, near, fine, pairs, spread, start, resid, corr, lower, wide, first, second, tall, twice, strip):
    level = Fine(pos)
    tall[...] = exact(near[...], spread[...])
    for i in range(16):
        value = tall[i * 16 + 2 : i * 16 + 14, :]
        twice[pl.ds(0, 12, stride=2), :] = value
        twice[pl.ds(1, 12, stride=2), :] = value
        wide[1 + 2 * i] = twice[...]
        wide[2 + 2 * i] = twice[...]
    clear(wide, XF)
    clear(first, XF)
    clear(second, XF)
    for k in range(16):
        start[k] = wide[9 + k][8:16]

    def body(x):
        c, around = level.around(wide, x)
        edge = c * ((1.0 - level.low) + (1.0 - level.high))
        value = 2.0 * fine[x] - (6.0 * c - (around + edge))
        held = jnp.where(level.scale(x) > 0.0, value, 0.0)
        resid[x] = held
        first[x + 1] = held * STEP

    over(XF, body)
    sweep(level, first, resid, second)
    corr[...] = second[1 : XF + 1]
    lower_of(level, second, resid, strip, pairs[...], lower)


def coarse(pos, blocks, corr, resid, tables, scratch):
    right1, left1, other1, right2, left2, other2, rows, double, grown, twice, first, second = scratch
    spread, merge, widen = tables
    level1 = Coarse(8 * pos[0] - 16, 256, X1, Y1, 4 * pos[1] - 14, 64, HALF)
    level2 = Coarse(4 * pos[0] - 8, 128, X2, Y2, 2 * pos[1] - 7, 32, HALF // 2)
    fine = Fine(pos)
    for x in range(X1):
        here = blocks[x // 8][x % 4]
        there = blocks[(x + X1) // 8][x % 4]
        if (x % 8) // 4:
            value = pltpu.roll(jnp.where(level1.left, there, here), HALF, 1)
        else:
            value = jnp.where(level1.left, here, there)
        right1[x] = value
        left1[x + 1] = value * STEP
    level1.join(left1)
    sweep(level1, left1, right1, other1)
    level1.join(other1)

    def down(k):
        total = None
        for a in range(2):
            c, near = level1.around(other1, 2 * k + a)
            value = right1[2 * k + a] - (6.0 * c - near)
            total = value if total is None else total + value
        double[...] = total
        rows[pl.ds(pl.multiple_of(k * Y2, Y2), Y2), :] = double[pl.ds(0, Y2, stride=2), :] + double[pl.ds(1, Y2, stride=2), :]

    over(X2, down, 1)
    rows[...] = exact(rows[...], merge)

    def begin(k):
        value = rows[pl.ds(pl.multiple_of(k * Y2, Y2), Y2), :]
        value = jnp.where(level2.scale(k) > 0.0, 0.5 * value, 0.0)
        right2[k] = value
        left2[k + 1] = value * STEP

    over(X2, begin, 5)
    level2.join(left2)
    sweep(level2, left2, right2, other2, 5)
    level2.join(other2)
    sweep(level2, other2, right2, left2, 5)
    level2.join(left2)
    sweep(level2, left2, right2, other2, 5)
    rows[...] = exact(other2[1 : X2 + 1].reshape(X2 * Y2, LANES), widen)

    def up(k):
        value = rows[pl.ds(pl.multiple_of(k * Y2, Y2), Y2), :]
        double[pl.ds(0, Y2, stride=2), :] = value
        double[pl.ds(1, Y2, stride=2), :] = value
        value = double[...]
        other1[1 + 2 * k] = other1[1 + 2 * k] + value
        other1[2 + 2 * k] = other1[2 + 2 * k] + value

    over(X2, up, 1)
    level1.join(other1)
    sweep(level1, other1, right1, left1)
    level1.join(left1)
    sweep(level1, left1, right1, other1)
    for k in range(16):
        x = 12 + k
        value = other1[1 + x % X1][10:26]
        grown[k * 16 : k * 16 + 16, :] = value if x < X1 else pltpu.roll(value, HALF, 1)
    grown[...] = exact(grown[...], spread)
    for i in range(16):
        value = grown[i * 16 : i * 16 + 12, :]
        twice[pl.ds(0, 12, stride=2), :] = value
        twice[pl.ds(1, 12, stride=2), :] = value
        first[1 + 2 * i] = corr[2 * i] + twice[...]
        first[2 + 2 * i] = corr[2 * i + 1] + twice[...]
    return fine


def turn_kernel(pos, b0, b1, b2, b3, b4, corr, resid, pairs, spread, merge, widen, after, lower, *scratch):
    strip, scratch = scratch[-1], scratch[:-1]
    tables = (spread[...], merge[...], widen[...])
    fine = coarse(pos, (b0, b1, b2, b3, b4), corr, resid, tables, scratch)
    first, second = scratch[-2:]
    sweep(fine, first, resid, second, 2, 3, 26)
    sweep(fine, second, resid, first, 4, 4, 24)
    sweep(fine, first, resid, second, 2, 5, 22)
    sweep(fine, second, resid, first, 4, 6, 20)
    for k in range(6, 26):
        after[k] = first[k + 1]
    for k in (0, 1, 2, 3, 4, 5, 26, 27, 28, 29, 30, 31):
        after[k] = jnp.zeros((YF, LANES), F32)
    lower_of(fine, first, resid, strip, pairs[...], lower)


def close_kernel(pos, b0, b1, b2, b3, b4, corr, resid, spread, merge, widen, start, out, *scratch):
    tables = (spread[...], merge[...], widen[...])
    fine = coarse(pos, (b0, b1, b2, b3, b4), corr, resid, tables, scratch)
    first, second = scratch[-2:]
    sweep(fine, first, resid, second, 2, 7, 18)
    sweep(fine, second, resid, first, 4, 8, 16)
    for k in range(16):
        out[k] = start[k] + first[9 + k][8:16]


def held(*shape):
    return pltpu.VMEM(shape, F32)


def shaped(*shape):
    return jax.ShapeDtypeStruct(shape, F32)


def inner():
    return [
        held(X1, Y1, LANES),
        held(X1 + 2, Y1, LANES),
        held(X1 + 2, Y1, LANES),
        held(X2, Y2, LANES),
        held(X2 + 2, Y2, LANES),
        held(X2 + 2, Y2, LANES),
        held(X2 * Y2, LANES),
        held(Y1, LANES),
        held(256, LANES),
        held(YF, LANES),
        held(XF + 2, YF, LANES),
        held(XF + 2, YF, LANES),
    ]


def many(body, name, count, shapes, scratch):
    return pl.pallas_call(
        body,
        name=name,
        in_specs=[SMEM] + [VMEM] * count,
        out_specs=[VMEM] * len(shapes),
        out_shape=shapes,
        scratch_shapes=scratch,
        compiler_params=PARAMS,
        interpret=INTERPRET,
    )


def opening(pos, near, fine, pairs, spread):
    shapes = [shaped(16, 8, LANES), shaped(XF, YF, LANES), shaped(XF, YF, LANES), shaped(16, LANES)]
    scratch = [held(XF + 2, YF, LANES)] * 3 + [held(256, LANES), held(YF, LANES), held(64, LANES)]
    return many(open_kernel, "opening", 4, shapes, scratch)(pos, near, fine, pairs, spread)


def turning(pos, blocks, corr, resid, tables):
    shapes = [shaped(XF, YF, LANES), shaped(16, LANES)]
    return many(turn_kernel, "turning", 11, shapes, inner() + [held(64, LANES)])(pos, *blocks, corr, resid, *tables)


def closing(pos, blocks, corr, resid, tables, start):
    return many(close_kernel, "closing", 11, [shaped(16, 8, LANES)], inner())(
        pos, *blocks, corr, resid, *tables[1:], start
    )[0]


def shifted(value, axes, size, step):
    return lax.ppermute(value, axes, [(i, i + step) for i in range(size) if 0 <= i + step < size])


def gather(lower, place):
    every = jnp.broadcast_to(lower[None], (YY, 16, LANES))
    every = lax.all_to_all(every, ("group", "gy"), 0, 0, tiled=True)
    every = jnp.pad(every, ((4, 4), (0, 0), (0, 0)))
    window = lax.dynamic_slice(every, (place, 0, 0), (9, 16, LANES))
    block = window.reshape(9, 4, 4, LANES).transpose(1, 0, 2, 3).reshape(4, 36, LANES)[:, 2:34]
    return [block if step == 0 else shifted(block, "gx", GX, step) for step in (2, 1, 0, -1, -2)]


def widened(fine):
    sides = ("group", "gy")
    tall = jnp.concatenate([shifted(fine, sides, YY, 1), fine, shifted(fine, sides, YY, -1)], axis=1)
    before = shifted(tall[8:16], "gx", GX, 1)
    behind = shifted(tall[0:8], "gx", GX, -1)
    return jnp.concatenate([before, tall, behind], axis=0)


def local(parent_mass, fine_mass, offsets):
    high, low, pairs, column, row, eigen = constants()
    spread = pairs.T
    spot = np.arange(LANES)
    merge = np.zeros((LANES, LANES), np.float32)
    merge[spot, spot % HALF // 2 + HALF * (spot // HALF)] = 1.0
    tables = (pairs, spread, jnp.asarray(merge, BF16), jnp.asarray(merge.T, BF16))
    pos = jnp.stack([lax.axis_index("gx"), lax.axis_index(("group", "gy"))]).astype(jnp.int32)
    wave = lax.dynamic_slice(eigen, (lax.axis_index(ALL),), (1,))
    wide = widened(fine_mass)
    got = swap(forward(offsets, parent_mass.reshape(NP, NP), fine_mass, high, low, pairs), FORE * LANES)
    got = swap(spectral(offsets, wave, got, high, low, column, row), BACK * LANES)
    near = near_back(offsets, got, high, low)
    start, resid, corr, lower = opening(pos, near, wide, pairs, spread)
    potential = whole_back(got, high, low)
    corr, lower = turning(pos, gather(lower, pos[1]), corr, resid, tables)
    out = closing(pos, gather(lower, pos[1]), corr, resid, tables, start)
    return (potential.reshape(WX, WY, NP), out)


def solution(mesh):
    spec = P("gx", ("group", "gy"), None)
    return jax.shard_map(
        local,
        mesh=mesh,
        in_specs=(spec, spec, P()),
        out_specs=(spec, spec),
        check_vma=False,
    )
```

```python
import math

import jax
import jax.numpy as jnp
import numpy as np
from jax import lax
from jax.experimental import pallas as pl
from jax.experimental.pallas import tpu as pltpu
from jax.sharding import PartitionSpec as P

NP = 512
CYCLES = 2
LEVELS = 3
SWEEPS = 2
COARSE_SWEEPS = 4

OMEGA = 6.0 / 7.0
F32 = jnp.float32
BF16 = jnp.bfloat16
ALL = ("group", "gy", "gx")
GX = 32
YY = 16
WX = NP // GX
WY = NP // YY
SX = 256
SY = 64
SZ = 64
HX = 4
HY = 6
LANES = 128
FORE = 5
BACK = 6


def split(x):
    high = x.astype(BF16)
    return high, (x - high.astype(F32)).astype(BF16)


def product(a, b, dims):
    def dot(u, v):
        return lax.dot_general(u, v, (dims, ((), ())), preferred_element_type=F32)

    return dot(a[0], b[0]) + (dot(a[0], b[1]) + dot(a[1], b[0]))


NN = ((1,), (0,))
NT = ((1,), (1,))


def forward_kernel(offsets, mass, fine, high, low, pairs, out, beside):
    for i in range(8):
        beside[8 * i : 8 * i + 8, :] = fine[2 * i] + fine[2 * i + 1]
    both = beside[pl.ds(0, 32, stride=2), :] + beside[pl.ds(1, 32, stride=2), :]
    first = both.astype(BF16)
    left = both - first.astype(F32)
    second = left.astype(BF16)
    third = (left - second.astype(F32)).astype(BF16)
    add = pairs[...]

    def dot(u):
        return lax.dot_general(u, add, (NN, ((), ())), preferred_element_type=F32)

    rest = dot(first) + (dot(second) + dot(third))
    rest = jnp.concatenate([rest, jnp.zeros((96, LANES), F32)], axis=0)
    rest = jnp.concatenate([rest, jnp.zeros((LANES, NP - LANES), F32)], axis=1)
    rest = pltpu.roll(rest, offsets[2], 1)
    table = (high[...], low[...])
    dense = product(table, split(mass[...]), NT)
    for c in range(4):
        out[pl.ds(c, NP, stride=FORE), :] = dense[:, c * LANES : (c + 1) * LANES]
    out[pl.ds(4, NP, stride=FORE), :] = product(table, split(rest), NT)


def place(group, amount, shift, total, value):
    amount = amount % LANES
    if amount:
        value = pltpu.roll(value, amount, 1)
    if total is None:
        return value
    return jnp.where(group == shift, value, total)


def plane_kernel(offsets, wave, got, high, low, column, row, out, plane0, plane1, plane2, plane3, rest):
    plane = (plane0, plane1, plane2, plane3)
    lane = lax.broadcasted_iota(jnp.int32, (GX, LANES), 1)
    group = lane // WY
    for a in range(4):
        for b in range(4):
            parts = [got[pl.ds((b * 4 + q) * GX * FORE + a, GX, stride=FORE), :] for q in range(4)]
            for p in range(4):
                total = None
                for q in range(4):
                    total = place(group, (q - p) * WY, q, total, parts[q])
                plane[b][pl.ds(a * 4 + p, GX, stride=WX), :] = total
    light = lane // 4
    parts = [got[pl.ds(q * GX * FORE + 4, GX, stride=FORE), :] for q in range(YY)]
    for p in range(8):
        total = jnp.zeros((GX, LANES), F32)
        for q in range(YY):
            total = place(light, (q - p) * 4, q, total, parts[q])
        rest[pl.ds(p, GX, stride=8), :] = total
    wide = jnp.concatenate([rest[0:SX, :], jnp.zeros((SX, NP - LANES), F32)], axis=1)
    wide = pltpu.roll(wide, offsets[1], 1)
    wide = jnp.concatenate([wide, jnp.zeros((NP - SX, NP), F32)], axis=0)
    wide = pltpu.roll(wide, offsets[0], 0)
    table = (high[...], low[...])
    half = product(table, split(jnp.concatenate([part[...] for part in plane], axis=1) + wide), NN)
    spectrum = product(split(half), table, NN)
    lam = column[...] + (row[...] + wave[0])
    spectrum = spectrum * jnp.where(lam > 0, (1.0 / float(NP**3)) / jnp.where(lam > 0, lam, 1.0), 0.0)
    half = product(split(spectrum), table, NN)
    whole = product(table, split(half), NN)
    for b in range(4):
        plane[b][...] = whole[:, b * LANES : (b + 1) * LANES]
    near = pltpu.roll(whole, (NP - offsets[0]) % NP, 0)[0:SX, :]
    near = pltpu.roll(near, (NP + HY - offsets[1]) % NP, 1)[:, 0:LANES]
    place_of = lax.broadcasted_iota(jnp.int32, (SX, LANES), 1)
    near = jnp.where(place_of < HY, near[:, HY : HY + 1], near)
    near = jnp.where(place_of >= HY + SY, near[:, HY + SY - 1 : HY + SY], near)
    rest[HX : HX + SX, :] = near
    rest[0:HX, :] = jnp.broadcast_to(near[0:1, :], (HX, LANES))
    rest[HX + SX : 2 * HX + SX, :] = jnp.broadcast_to(near[SX - 1 : SX, :], (HX, LANES))
    for a in range(4):
        for b in range(4):
            parts = [plane[b][pl.ds(a * 4 + p, GX, stride=WX), :] for p in range(4)]
            for q in range(4):
                total = None
                for p in range(4):
                    total = place(group, (p - q) * WY, p, total, parts[p])
                out[pl.ds((b * 4 + q) * GX * BACK + a, GX, stride=BACK), :] = total
    wing = lane // 16
    for h in range(2):
        parts = [rest[pl.ds(h * 8 + p, GX, stride=8), :] for p in range(8)]
        for q in range(YY):
            total = None
            for p in range(8):
                total = place(wing, p * 16 - 4 * q, p, total, parts[p])
            out[pl.ds(q * GX * BACK + 4 + h, GX, stride=BACK), :] = total


def near_kernel(offsets, got, high, low, out):
    table = (high[...], low[...])
    back = (NP - offsets[2]) % NP
    for h in range(2):
        turned = got[pl.ds(4 + h, NP, stride=BACK), :].T
        rows = product(split(turned), table, NN)
        out[h * LANES : (h + 1) * LANES, :] = pltpu.roll(rows, back, 1)[:, 0:LANES]


def whole_kernel(got, high, low, out):
    table = (high[...], low[...])
    for c in range(4):
        turned = got[pl.ds(c, NP, stride=BACK), :].T
        out[c * LANES : (c + 1) * LANES, :] = product(split(turned), table, NN)


def cas_tables():
    wave = np.arange(NP)
    angle = (wave[:, None] * wave[None, :] % NP) * (2.0 * np.pi / NP)
    return jnp.asarray((np.cos(angle) + np.sin(angle)).astype(np.float32))


def eigenvalues():
    sine = np.sin(np.arange(NP) * (np.pi / NP))
    return (4.0 * sine * sine).astype(np.float32)


VMEM = pl.BlockSpec(memory_space=pltpu.VMEM)
SMEM = pl.BlockSpec(memory_space=pltpu.SMEM)
BIG = 56 * 1024 * 1024
SMALL = 32 * 1024 * 1024
INTERPRET = False


def call(body, name, ins, shape, scratch=(), limit=SMALL):
    return pl.pallas_call(
        body,
        name=name,
        in_specs=ins,
        out_specs=VMEM,
        out_shape=shape,
        scratch_shapes=list(scratch),
        compiler_params=pltpu.CompilerParams(vmem_limit_bytes=limit),
        interpret=INTERPRET,
    )


def forward(offsets, mass, fine, high, low, pairs):
    return call(forward_kernel, "forward", [SMEM] + [VMEM] * 5, shaped(NP * FORE, LANES), [pltpu.VMEM((64, LANES), F32)], BIG)(
        offsets, mass, fine, high, low, pairs
    )


def spectral(offsets, wave, got, high, low, column, row):
    return call(
        plane_kernel,
        "plane",
        [SMEM, SMEM] + [VMEM] * 5,
        shaped(NP * BACK, LANES),
        [pltpu.VMEM((NP, LANES), F32)] * 4 + [pltpu.VMEM((SX + 8, LANES), F32)],
        BIG,
    )(offsets, wave, got, high, low, column, row)


def near_back(offsets, got, high, low):
    return call(near_kernel, "near", [SMEM] + [VMEM] * 3, shaped(256, LANES))(offsets, got, high, low)


def whole_back(got, high, low):
    return call(whole_kernel, "whole", [VMEM] * 3, shaped(NP, NP))(got, high, low)


def swap(piece, lanes):
    piece = piece.reshape(NP, 1, lanes)
    piece = lax.all_to_all(piece, ALL, 0, 0, tiled=True).reshape(NP * lanes // LANES, LANES)
    return pltpu.with_memory_space_constraint(piece, pltpu.VMEM)


def constants():
    high, low = split(cas_tables())
    pairs = np.zeros((LANES, LANES), np.float32)
    pairs[np.arange(LANES), np.arange(LANES) // 2] = 1.0
    eigen = eigenvalues()
    return high, low, jnp.asarray(pairs, BF16), jnp.asarray(eigen[:, None]), jnp.asarray(eigen[None, :]), jnp.asarray(eigen)


XF = 32
YF = 24
X1 = 20
Y1 = 32
X2 = 10
Y2 = 16
HALF = 64
STEP = 1.0 / 7.0


def exact(value, table):
    first = value.astype(BF16)
    left = value - first.astype(F32)
    second = left.astype(BF16)
    third = (left - second.astype(F32)).astype(BF16)

    def dot(u):
        return lax.dot_general(u, table, (NN, ((), ())), preferred_element_type=F32)

    return dot(first) + (dot(second) + dot(third))


def over(count, body, per=4, base=0):
    def group(t, carry):
        for k in range(per):
            body(base + t * per + k)
        return carry

    lax.fori_loop(0, count // per, group, 0)


def lanes_of(rows):
    return lax.broadcasted_iota(jnp.int32, (rows, LANES), 1)


def rows_of(rows):
    return lax.broadcasted_iota(jnp.int32, (rows, LANES), 0)


def inside(place, count):
    return jnp.where((place >= 0) & (place < count), 1.0, 0.0).astype(F32)


class Fine:
    def __init__(self, pos):
        self.first = 16 * pos[0] - 8
        self.count = 512
        self.x = XF
        y = rows_of(YF) + (8 * pos[1] - 8)
        self.mask = jnp.where((y >= 0) & (y < 128), STEP, 0.0)
        lane = lanes_of(YF)
        self.low = jnp.where(lane == 0, 0.0, 1.0)
        self.high = jnp.where(lane == LANES - 1, 0.0, 1.0)

    def scale(self, x):
        return self.mask * inside(self.first + x, self.count)

    def around(self, ref, x):
        c = ref[x + 1]
        near = ref[x] + ref[x + 2]
        near = near + (pltpu.roll(c, 1, 0) + pltpu.roll(c, YF - 1, 0))
        near = near + (pltpu.roll(c, 1, 1) * self.low + pltpu.roll(c, LANES - 1, 1) * self.high)
        return c, near


class Coarse:
    def __init__(self, first, count, x, y, first_y, count_y, z):
        self.first = first
        self.count = count
        self.x = x
        row = rows_of(y) + first_y
        lane = lanes_of(y)
        self.y = y
        self.left = lane < HALF
        place = lane % HALF
        self.mask = jnp.where((place < z) & (row >= 0) & (row < count_y), STEP, 0.0)
        self.low = jnp.where(place == 0, 0.0, 1.0)
        self.high = jnp.where(place == HALF - 1, 0.0, 1.0)

    def scale(self, x):
        here = inside(self.first + x, self.count)
        there = inside(self.first + self.x + x, self.count)
        return self.mask * jnp.where(self.left, here, there)

    def around(self, ref, x):
        c = ref[x + 1]
        near = ref[x] + ref[x + 2]
        near = near + (pltpu.roll(c, 1, 0) + pltpu.roll(c, self.y - 1, 0))
        near = near + (pltpu.roll(c, 1, 1) * self.low + pltpu.roll(c, LANES - 1, 1) * self.high)
        return c, near

    def join(self, ref):
        ref[0] = jnp.where(self.left, 0.0, pltpu.roll(ref[self.x], HALF, 1))
        ref[self.x + 1] = jnp.where(self.left, pltpu.roll(ref[1], HALF, 1), 0.0)


def sweep(level, source, right, target, per=4, base=0, count=None):
    def body(x):
        c, near = level.around(source, x)
        target[x + 1] = (right[x] + (c + near)) * level.scale(x)

    over(level.x if count is None else count, body, per, base)


def clear(ref, size):
    ref[0] = jnp.zeros(ref.shape[1:], F32)
    ref[size + 1] = jnp.zeros(ref.shape[1:], F32)


def lower_of(level, corr, resid, strip, pairs, out):
    def left(x):
        c, near = level.around(corr, x)
        return (resid[x] - (6.0 * c - near))[8:16]

    for k in range(8):
        strip[8 * k : 8 * k + 8, :] = left(8 + 2 * k) + left(9 + 2 * k)
    both = strip[pl.ds(0, 32, stride=2), :] + strip[pl.ds(1, 32, stride=2), :]
    small = 0.5 * exact(both, pairs)
    out[...] = small[0:16] + pltpu.roll(small[16:32], 64, 1)


def open_kernel(pos, near, fine, pairs, spread, start, resid, corr, lower, wide, first, second, tall, twice, strip):
    level = Fine(pos)
    tall[...] = exact(near[...], spread[...])
    for i in range(16):
        value = tall[i * 16 + 2 : i * 16 + 14, :]
        twice[pl.ds(0, 12, stride=2), :] = value
        twice[pl.ds(1, 12, stride=2), :] = value
        wide[1 + 2 * i] = twice[...]
        wide[2 + 2 * i] = twice[...]
    clear(wide, XF)
    clear(first, XF)
    clear(second, XF)
    for k in range(16):
        start[k] = wide[9 + k][8:16]

    def body(x):
        c, around = level.around(wide, x)
        edge = c * ((1.0 - level.low) + (1.0 - level.high))
        value = 2.0 * fine[x] - (6.0 * c - (around + edge))
        held = jnp.where(level.scale(x) > 0.0, value, 0.0)
        resid[x] = held
        first[x + 1] = held * STEP

    over(XF, body)
    sweep(level, first, resid, second)
    corr[...] = second[1 : XF + 1]
    lower_of(level, second, resid, strip, pairs[...], lower)


def coarse(pos, blocks, corr, resid, tables, scratch):
    right1, left1, other1, right2, left2, other2, rows, double, grown, twice, first, second = scratch
    spread, merge, widen = tables
    level1 = Coarse(8 * pos[0] - 16, 256, X1, Y1, 4 * pos[1] - 14, 64, HALF)
    level2 = Coarse(4 * pos[0] - 8, 128, X2, Y2, 2 * pos[1] - 7, 32, HALF // 2)
    fine = Fine(pos)
    for x in range(X1):
        here = blocks[x // 8][x % 4]
        there = blocks[(x + X1) // 8][x % 4]
        if (x % 8) // 4:
            value = pltpu.roll(jnp.where(level1.left, there, here), HALF, 1)
        else:
            value = jnp.where(level1.left, here, there)
        right1[x] = value
        left1[x + 1] = value * STEP
    level1.join(left1)
    sweep(level1, left1, right1, other1)
    level1.join(other1)

    def down(k):
        total = None
        for a in range(2):
            c, near = level1.around(other1, 2 * k + a)
            value = right1[2 * k + a] - (6.0 * c - near)
            total = value if total is None else total + value
        double[...] = total
        rows[pl.ds(pl.multiple_of(k * Y2, Y2), Y2), :] = double[pl.ds(0, Y2, stride=2), :] + double[pl.ds(1, Y2, stride=2), :]

    over(X2, down, 1)
    rows[...] = exact(rows[...], merge)

    def begin(k):
        value = rows[pl.ds(pl.multiple_of(k * Y2, Y2), Y2), :]
        value = jnp.where(level2.scale(k) > 0.0, 0.5 * value, 0.0)
        right2[k] = value
        left2[k + 1] = value * STEP

    over(X2, begin, 5)
    level2.join(left2)
    sweep(level2, left2, right2, other2, 5)
    level2.join(other2)
    sweep(level2, other2, right2, left2, 5)
    level2.join(left2)
    sweep(level2, left2, right2, other2, 5)
    rows[...] = exact(other2[1 : X2 + 1].reshape(X2 * Y2, LANES), widen)

    def up(k):
        value = rows[pl.ds(pl.multiple_of(k * Y2, Y2), Y2), :]
        double[pl.ds(0, Y2, stride=2), :] = value
        double[pl.ds(1, Y2, stride=2), :] = value
        value = double[...]
        other1[1 + 2 * k] = other1[1 + 2 * k] + value
        other1[2 + 2 * k] = other1[2 + 2 * k] + value

    over(X2, up, 1)
    level1.join(other1)
    sweep(level1, other1, right1, left1)
    level1.join(left1)
    sweep(level1, left1, right1, other1)
    for k in range(16):
        x = 12 + k
        value = other1[1 + x % X1][10:26]
        grown[k * 16 : k * 16 + 16, :] = value if x < X1 else pltpu.roll(value, HALF, 1)
    grown[...] = exact(grown[...], spread)
    for i in range(16):
        value = grown[i * 16 : i * 16 + 12, :]
        twice[pl.ds(0, 12, stride=2), :] = value
        twice[pl.ds(1, 12, stride=2), :] = value
        first[1 + 2 * i] = corr[2 * i] + twice[...]
        first[2 + 2 * i] = corr[2 * i + 1] + twice[...]
    return fine


def turn_kernel(pos, b0, b1, b2, b3, b4, corr, resid, pairs, spread, merge, widen, after, lower, *scratch):
    strip, scratch = scratch[-1], scratch[:-1]
    tables = (spread[...], merge[...], widen[...])
    fine = coarse(pos, (b0, b1, b2, b3, b4), corr, resid, tables, scratch)
    first, second = scratch[-2:]
    sweep(fine, first, resid, second, 2, 3, 26)
    sweep(fine, second, resid, first, 4, 4, 24)
    sweep(fine, first, resid, second, 2, 5, 22)
    sweep(fine, second, resid, first, 4, 6, 20)
    for k in range(6, 26):
        after[k] = first[k + 1]
    for k in (0, 1, 2, 3, 4, 5, 26, 27, 28, 29, 30, 31):
        after[k] = jnp.zeros((YF, LANES), F32)
    lower_of(fine, first, resid, strip, pairs[...], lower)


def close_kernel(pos, b0, b1, b2, b3, b4, corr, resid, spread, merge, widen, start, out, *scratch):
    tables = (spread[...], merge[...], widen[...])
    fine = coarse(pos, (b0, b1, b2, b3, b4), corr, resid, tables, scratch)
    first, second = scratch[-2:]
    sweep(fine, first, resid, second, 2, 7, 18)
    sweep(fine, second, resid, first, 4, 8, 16)
    for k in range(16):
        out[k] = start[k] + first[9 + k][8:16]


def held(*shape):
    return pltpu.VMEM(shape, F32)


def shaped(*shape):
    return jax.ShapeDtypeStruct(shape, F32)


def inner():
    return [
        held(X1, Y1, LANES),
        held(X1 + 2, Y1, LANES),
        held(X1 + 2, Y1, LANES),
        held(X2, Y2, LANES),
        held(X2 + 2, Y2, LANES),
        held(X2 + 2, Y2, LANES),
        held(X2 * Y2, LANES),
        held(Y1, LANES),
        held(256, LANES),
        held(YF, LANES),
        held(XF + 2, YF, LANES),
        held(XF + 2, YF, LANES),
    ]


def many(body, name, count, shapes, scratch, limit=SMALL):
    return pl.pallas_call(
        body,
        name=name,
        in_specs=[SMEM] + [VMEM] * count,
        out_specs=[VMEM] * len(shapes),
        out_shape=shapes,
        scratch_shapes=scratch,
        compiler_params=pltpu.CompilerParams(vmem_limit_bytes=limit),
        interpret=INTERPRET,
    )


def opening(pos, near, fine, pairs, spread):
    shapes = [shaped(16, 8, LANES), shaped(XF, YF, LANES), shaped(XF, YF, LANES), shaped(16, LANES)]
    scratch = [held(XF + 2, YF, LANES)] * 3 + [held(256, LANES), held(YF, LANES), held(64, LANES)]
    return many(open_kernel, "opening", 4, shapes, scratch)(pos, near, fine, pairs, spread)


def turning(pos, blocks, corr, resid, tables):
    shapes = [shaped(XF, YF, LANES), shaped(16, LANES)]
    return many(turn_kernel, "turning", 11, shapes, inner() + [held(64, LANES)])(pos, *blocks, corr, resid, *tables)


def closing(pos, blocks, corr, resid, tables, start):
    return many(close_kernel, "closing", 11, [shaped(16, 8, LANES)], inner())(
        pos, *blocks, corr, resid, *tables[1:], start
    )[0]


def shifted(value, axes, size, step):
    return lax.ppermute(value, axes, [(i, i + step) for i in range(size) if 0 <= i + step < size])


def gather(lower, place):
    every = jnp.broadcast_to(lower[None], (YY, 16, LANES))
    every = lax.all_to_all(every, ("group", "gy"), 0, 0, tiled=True)
    every = jnp.pad(every, ((4, 4), (0, 0), (0, 0)))
    window = lax.dynamic_slice(every, (place, 0, 0), (9, 16, LANES))
    block = window.reshape(9, 4, 4, LANES).transpose(1, 0, 2, 3).reshape(4, 36, LANES)[:, 2:34]
    blocks = [block if step == 0 else shifted(block, "gx", GX, step) for step in (2, 1, 0, -1, -2)]
    return [pltpu.with_memory_space_constraint(block, pltpu.VMEM) for block in blocks]


def taller(fine):
    sides = ("group", "gy")
    return jnp.concatenate([shifted(fine, sides, YY, 1), fine, shifted(fine, sides, YY, -1)], axis=1)


def wider(tall):
    before = shifted(tall[8:16], "gx", GX, 1)
    behind = shifted(tall[0:8], "gx", GX, -1)
    return pltpu.with_memory_space_constraint(jnp.concatenate([before, tall, behind], axis=0), pltpu.VMEM)


def local(parent_mass, fine_mass, offsets):
    high, low, pairs, column, row, eigen = constants()
    spread = pairs.T
    spot = np.arange(LANES)
    merge = np.zeros((LANES, LANES), np.float32)
    merge[spot, spot % HALF // 2 + HALF * (spot // HALF)] = 1.0
    tables = (pairs, spread, jnp.asarray(merge, BF16), jnp.asarray(merge.T, BF16))
    pos = jnp.stack([lax.axis_index("gx"), lax.axis_index(("group", "gy"))]).astype(jnp.int32)
    wave = lax.dynamic_slice(eigen, (lax.axis_index(ALL),), (1,))
    tall = taller(fine_mass)
    got = swap(forward(offsets, parent_mass.reshape(NP, NP), fine_mass, high, low, pairs), FORE * LANES)
    got, tall = lax.optimization_barrier((got, tall))
    wide = wider(tall)
    got = swap(spectral(offsets, wave, got, high, low, column, row), BACK * LANES)
    near = near_back(offsets, got, high, low)
    start, resid, corr, lower = opening(pos, near, wide, pairs, spread)
    potential = whole_back(got, high, low)
    corr, lower = turning(pos, gather(lower, pos[1]), corr, resid, tables)
    out = closing(pos, gather(lower, pos[1]), corr, resid, tables, start)
    return (potential.reshape(WX, WY, NP), out)


def solution(mesh):
    spec = P("gx", ("group", "gy"), None)
    return jax.shard_map(
        local,
        mesh=mesh,
        in_specs=(spec, spec, P()),
        out_specs=(spec, spec),
        check_vma=False,
    )
```

```python
import math

import jax
import jax.numpy as jnp
import numpy as np
from jax import lax
from jax.experimental import pallas as pl
from jax.experimental.pallas import tpu as pltpu
from jax.sharding import PartitionSpec as P

NP = 512
CYCLES = 2
LEVELS = 3
SWEEPS = 2
COARSE_SWEEPS = 4

OMEGA = 6.0 / 7.0
F32 = jnp.float32
BF16 = jnp.bfloat16
ALL = ("group", "gy", "gx")
GX = 32
YY = 16
WX = NP // GX
WY = NP // YY
SX = 256
SY = 64
SZ = 64
HX = 4
HY = 6
LANES = 128
FORE = 5
BACK = 6


def split(x):
    high = x.astype(BF16)
    return high, (x - high.astype(F32)).astype(BF16)


def product(a, b, dims):
    def dot(u, v):
        return lax.dot_general(u, v, (dims, ((), ())), preferred_element_type=F32)

    return dot(a[0], b[0]) + (dot(a[0], b[1]) + dot(a[1], b[0]))


NN = ((1,), (0,))
NT = ((1,), (1,))


def forward_kernel(offsets, mass, fine, high, low, pairs, out, beside):
    for i in range(8):
        beside[8 * i : 8 * i + 8, :] = fine[2 * i] + fine[2 * i + 1]
    both = beside[pl.ds(0, 32, stride=2), :] + beside[pl.ds(1, 32, stride=2), :]
    first = both.astype(BF16)
    left = both - first.astype(F32)
    second = left.astype(BF16)
    third = (left - second.astype(F32)).astype(BF16)
    add = pairs[...]

    def dot(u):
        return lax.dot_general(u, add, (NN, ((), ())), preferred_element_type=F32)

    rest = dot(first) + (dot(second) + dot(third))
    rest = jnp.concatenate([rest, jnp.zeros((96, LANES), F32)], axis=0)
    rest = jnp.concatenate([rest, jnp.zeros((LANES, NP - LANES), F32)], axis=1)
    rest = pltpu.roll(rest, offsets[2], 1)
    table = (high[...], low[...])
    dense = product(table, split(mass[...]), NT)
    for c in range(4):
        out[pl.ds(c, NP, stride=FORE), :] = dense[:, c * LANES : (c + 1) * LANES]
    out[pl.ds(4, NP, stride=FORE), :] = product(table, split(rest), NT)


def place(group, amount, shift, total, value):
    amount = amount % LANES
    if amount:
        value = pltpu.roll(value, amount, 1)
    if total is None:
        return value
    return jnp.where(group == shift, value, total)


def plane_kernel(offsets, wave, got, high, low, column, row, out, plane0, plane1, plane2, plane3, rest):
    plane = (plane0, plane1, plane2, plane3)
    lane = lax.broadcasted_iota(jnp.int32, (GX, LANES), 1)
    group = lane // WY
    for a in range(4):
        for b in range(4):
            parts = [got[pl.ds((b * 4 + q) * GX * FORE + a, GX, stride=FORE), :] for q in range(4)]
            for p in range(4):
                total = None
                for q in range(4):
                    total = place(group, (q - p) * WY, q, total, parts[q])
                plane[b][pl.ds(a * 4 + p, GX, stride=WX), :] = total
    light = lane // 4
    parts = [got[pl.ds(q * GX * FORE + 4, GX, stride=FORE), :] for q in range(YY)]
    for p in range(8):
        total = jnp.zeros((GX, LANES), F32)
        for q in range(YY):
            total = place(light, (q - p) * 4, q, total, parts[q])
        rest[pl.ds(p, GX, stride=8), :] = total
    wide = jnp.concatenate([rest[0:SX, :], jnp.zeros((SX, NP - LANES), F32)], axis=1)
    wide = pltpu.roll(wide, offsets[1], 1)
    wide = jnp.concatenate([wide, jnp.zeros((NP - SX, NP), F32)], axis=0)
    wide = pltpu.roll(wide, offsets[0], 0)
    table = (high[...], low[...])
    half = product(table, split(jnp.concatenate([part[...] for part in plane], axis=1) + wide), NN)
    spectrum = product(split(half), table, NN)
    lam = column[...] + (row[...] + wave[0])
    spectrum = spectrum * jnp.where(lam > 0, (1.0 / float(NP**3)) / jnp.where(lam > 0, lam, 1.0), 0.0)
    half = product(split(spectrum), table, NN)
    whole = product(table, split(half), NN)
    for b in range(4):
        plane[b][...] = whole[:, b * LANES : (b + 1) * LANES]
    near = pltpu.roll(whole, (NP - offsets[0]) % NP, 0)[0:SX, :]
    near = pltpu.roll(near, (NP + HY - offsets[1]) % NP, 1)[:, 0:LANES]
    place_of = lax.broadcasted_iota(jnp.int32, (SX, LANES), 1)
    near = jnp.where(place_of < HY, near[:, HY : HY + 1], near)
    near = jnp.where(place_of >= HY + SY, near[:, HY + SY - 1 : HY + SY], near)
    rest[HX : HX + SX, :] = near
    rest[0:HX, :] = jnp.broadcast_to(near[0:1, :], (HX, LANES))
    rest[HX + SX : 2 * HX + SX, :] = jnp.broadcast_to(near[SX - 1 : SX, :], (HX, LANES))
    for a in range(4):
        for b in range(4):
            parts = [plane[b][pl.ds(a * 4 + p, GX, stride=WX), :] for p in range(4)]
            for q in range(4):
                total = None
                for p in range(4):
                    total = place(group, (p - q) * WY, p, total, parts[p])
                out[pl.ds((b * 4 + q) * GX * BACK + a, GX, stride=BACK), :] = total
    wing = lane // 16
    for h in range(2):
        parts = [rest[pl.ds(h * 8 + p, GX, stride=8), :] for p in range(8)]
        for q in range(YY):
            total = None
            for p in range(8):
                total = place(wing, p * 16 - 4 * q, p, total, parts[p])
            out[pl.ds(q * GX * BACK + 4 + h, GX, stride=BACK), :] = total


def near_kernel(offsets, got, high, low, out):
    table = (high[...], low[...])
    back = (NP - offsets[2]) % NP
    for h in range(2):
        turned = got[pl.ds(4 + h, NP, stride=BACK), :].T
        rows = product(split(turned), table, NN)
        out[h * LANES : (h + 1) * LANES, :] = pltpu.roll(rows, back, 1)[:, 0:LANES]


def whole_kernel(got, high, low, out):
    table = (high[...], low[...])
    for c in range(4):
        turned = got[pl.ds(c, NP, stride=BACK), :].T
        out[c * LANES : (c + 1) * LANES, :] = product(split(turned), table, NN)


def cas_tables():
    wave = np.arange(NP)
    angle = (wave[:, None] * wave[None, :] % NP) * (2.0 * np.pi / NP)
    return jnp.asarray((np.cos(angle) + np.sin(angle)).astype(np.float32))


def eigenvalues():
    sine = np.sin(np.arange(NP) * (np.pi / NP))
    return (4.0 * sine * sine).astype(np.float32)


VMEM = pl.BlockSpec(memory_space=pltpu.VMEM)
SMEM = pl.BlockSpec(memory_space=pltpu.SMEM)
BIG = 56 * 1024 * 1024
SMALL = 32 * 1024 * 1024
INTERPRET = False


def call(body, name, ins, shape, scratch=(), limit=SMALL):
    return pl.pallas_call(
        body,
        name=name,
        in_specs=ins,
        out_specs=VMEM,
        out_shape=shape,
        scratch_shapes=list(scratch),
        compiler_params=pltpu.CompilerParams(vmem_limit_bytes=limit),
        interpret=INTERPRET,
    )


def forward(offsets, mass, fine, high, low, pairs):
    return call(forward_kernel, "forward", [SMEM] + [VMEM] * 5, shaped(NP * FORE, LANES), [pltpu.VMEM((64, LANES), F32)], BIG)(
        offsets, mass, fine, high, low, pairs
    )


def spectral(offsets, wave, got, high, low, column, row):
    return call(
        plane_kernel,
        "plane",
        [SMEM, SMEM] + [VMEM] * 5,
        shaped(NP * BACK, LANES),
        [pltpu.VMEM((NP, LANES), F32)] * 4 + [pltpu.VMEM((SX + 8, LANES), F32)],
        BIG,
    )(offsets, wave, got, high, low, column, row)


def near_back(offsets, got, high, low):
    return call(near_kernel, "near", [SMEM] + [VMEM] * 3, shaped(256, LANES))(offsets, got, high, low)


def whole_back(got, high, low):
    return call(whole_kernel, "whole", [VMEM] * 3, shaped(NP, NP))(got, high, low)


def swap(piece, lanes):
    piece = piece.reshape(NP, 1, lanes)
    piece = lax.all_to_all(piece, ALL, 0, 0, tiled=True).reshape(NP * lanes // LANES, LANES)
    return pltpu.with_memory_space_constraint(piece, pltpu.VMEM)


def constants():
    high, low = split(cas_tables())
    pairs = np.zeros((LANES, LANES), np.float32)
    pairs[np.arange(LANES), np.arange(LANES) // 2] = 1.0
    eigen = eigenvalues()
    return high, low, jnp.asarray(pairs, BF16), jnp.asarray(eigen[:, None]), jnp.asarray(eigen[None, :]), jnp.asarray(eigen)


XF = 32
YF = 24
X1 = 20
Y1 = 32
X2 = 10
Y2 = 16
HALF = 64
STEP = 1.0 / 7.0


def exact(value, table):
    first = value.astype(BF16)
    left = value - first.astype(F32)
    second = left.astype(BF16)
    third = (left - second.astype(F32)).astype(BF16)

    def dot(u):
        return lax.dot_general(u, table, (NN, ((), ())), preferred_element_type=F32)

    return dot(first) + (dot(second) + dot(third))


def over(count, body, per=4, base=0):
    def group(t, carry):
        for k in range(per):
            body(base + t * per + k)
        return carry

    lax.fori_loop(0, count // per, group, 0)


def lanes_of(rows):
    return lax.broadcasted_iota(jnp.int32, (rows, LANES), 1)


def rows_of(rows):
    return lax.broadcasted_iota(jnp.int32, (rows, LANES), 0)


def inside(place, count):
    return jnp.where((place >= 0) & (place < count), 1.0, 0.0).astype(F32)


class Fine:
    def __init__(self, pos):
        self.first = 16 * pos[0] - 8
        self.count = 512
        self.x = XF
        y = rows_of(YF) + (8 * pos[1] - 8)
        self.mask = jnp.where((y >= 0) & (y < 128), STEP, 0.0)
        lane = lanes_of(YF)
        self.low = jnp.where(lane == 0, 0.0, 1.0)
        self.high = jnp.where(lane == LANES - 1, 0.0, 1.0)

    def scale(self, x):
        return self.mask * inside(self.first + x, self.count)

    def around(self, ref, x):
        c = ref[x + 1]
        near = ref[x] + ref[x + 2]
        near = near + (pltpu.roll(c, 1, 0) + pltpu.roll(c, YF - 1, 0))
        near = near + (pltpu.roll(c, 1, 1) * self.low + pltpu.roll(c, LANES - 1, 1) * self.high)
        return c, near


class Coarse:
    def __init__(self, first, count, x, y, first_y, count_y, z):
        self.first = first
        self.count = count
        self.x = x
        row = rows_of(y) + first_y
        lane = lanes_of(y)
        self.y = y
        self.left = lane < HALF
        place = lane % HALF
        self.mask = jnp.where((place < z) & (row >= 0) & (row < count_y), STEP, 0.0)
        self.low = jnp.where(place == 0, 0.0, 1.0)
        self.high = jnp.where(place == HALF - 1, 0.0, 1.0)

    def scale(self, x):
        here = inside(self.first + x, self.count)
        there = inside(self.first + self.x + x, self.count)
        return self.mask * jnp.where(self.left, here, there)

    def around(self, ref, x):
        c = ref[x + 1]
        near = ref[x] + ref[x + 2]
        near = near + (pltpu.roll(c, 1, 0) + pltpu.roll(c, self.y - 1, 0))
        near = near + (pltpu.roll(c, 1, 1) * self.low + pltpu.roll(c, LANES - 1, 1) * self.high)
        return c, near

    def join(self, ref):
        ref[0] = jnp.where(self.left, 0.0, pltpu.roll(ref[self.x], HALF, 1))
        ref[self.x + 1] = jnp.where(self.left, pltpu.roll(ref[1], HALF, 1), 0.0)


def sweep(level, source, right, target, per=4, base=0, count=None):
    def body(x):
        c, near = level.around(source, x)
        target[x + 1] = (right[x] + (c + near)) * level.scale(x)

    over(level.x if count is None else count, body, per, base)


def clear(ref, size):
    ref[0] = jnp.zeros(ref.shape[1:], F32)
    ref[size + 1] = jnp.zeros(ref.shape[1:], F32)


def lower_of(level, corr, resid, strip, pairs, out):
    def left(x):
        c, near = level.around(corr, x)
        return (resid[x] - (6.0 * c - near))[8:16]

    for k in range(8):
        strip[8 * k : 8 * k + 8, :] = left(8 + 2 * k) + left(9 + 2 * k)
    both = strip[pl.ds(0, 32, stride=2), :] + strip[pl.ds(1, 32, stride=2), :]
    small = 0.5 * exact(both, pairs)
    out[...] = small[0:16] + pltpu.roll(small[16:32], 64, 1)


def open_kernel(pos, near, fine, pairs, spread, start, resid, corr, lower, wide, first, second, tall, twice, strip):
    level = Fine(pos)
    tall[...] = exact(near[...], spread[...])
    for i in range(16):
        value = tall[i * 16 + 2 : i * 16 + 14, :]
        twice[pl.ds(0, 12, stride=2), :] = value
        twice[pl.ds(1, 12, stride=2), :] = value
        wide[1 + 2 * i] = twice[...]
        wide[2 + 2 * i] = twice[...]
    clear(wide, XF)
    clear(first, XF)
    clear(second, XF)
    for k in range(16):
        start[k] = wide[9 + k][8:16]

    def body(x):
        c, around = level.around(wide, x)
        edge = c * ((1.0 - level.low) + (1.0 - level.high))
        value = 2.0 * fine[x] - (6.0 * c - (around + edge))
        held = jnp.where(level.scale(x) > 0.0, value, 0.0)
        resid[x] = held
        first[x + 1] = held * STEP

    over(XF, body)
    sweep(level, first, resid, second)
    corr[...] = second[1 : XF + 1]
    lower_of(level, second, resid, strip, pairs[...], lower)


def coarse(pos, blocks, corr, resid, tables, scratch):
    right1, left1, other1, right2, left2, other2, rows, double, grown, twice, first, second = scratch
    spread, merge, widen = tables
    level1 = Coarse(8 * pos[0] - 16, 256, X1, Y1, 4 * pos[1] - 14, 64, HALF)
    level2 = Coarse(4 * pos[0] - 8, 128, X2, Y2, 2 * pos[1] - 7, 32, HALF // 2)
    fine = Fine(pos)
    for x in range(X1):
        here = blocks[x // 8][x % 4]
        there = blocks[(x + X1) // 8][x % 4]
        if (x % 8) // 4:
            value = pltpu.roll(jnp.where(level1.left, there, here), HALF, 1)
        else:
            value = jnp.where(level1.left, here, there)
        right1[x] = value
        left1[x + 1] = value * STEP
    level1.join(left1)
    sweep(level1, left1, right1, other1)
    level1.join(other1)

    def down(k):
        total = None
        for a in range(2):
            c, near = level1.around(other1, 2 * k + a)
            value = right1[2 * k + a] - (6.0 * c - near)
            total = value if total is None else total + value
        double[...] = total
        rows[pl.ds(pl.multiple_of(k * Y2, Y2), Y2), :] = double[pl.ds(0, Y2, stride=2), :] + double[pl.ds(1, Y2, stride=2), :]

    over(X2, down, 1)
    rows[...] = exact(rows[...], merge)

    def begin(k):
        value = rows[pl.ds(pl.multiple_of(k * Y2, Y2), Y2), :]
        value = jnp.where(level2.scale(k) > 0.0, 0.5 * value, 0.0)
        right2[k] = value
        left2[k + 1] = value * STEP

    over(X2, begin, 5)
    level2.join(left2)
    sweep(level2, left2, right2, other2, 5)
    level2.join(other2)
    sweep(level2, other2, right2, left2, 5)
    level2.join(left2)
    sweep(level2, left2, right2, other2, 5)
    rows[...] = exact(other2[1 : X2 + 1].reshape(X2 * Y2, LANES), widen)

    def up(k):
        value = rows[pl.ds(pl.multiple_of(k * Y2, Y2), Y2), :]
        double[pl.ds(0, Y2, stride=2), :] = value
        double[pl.ds(1, Y2, stride=2), :] = value
        value = double[...]
        other1[1 + 2 * k] = other1[1 + 2 * k] + value
        other1[2 + 2 * k] = other1[2 + 2 * k] + value

    over(X2, up, 1)
    level1.join(other1)
    sweep(level1, other1, right1, left1)
    level1.join(left1)
    sweep(level1, left1, right1, other1)
    for k in range(16):
        x = 12 + k
        value = other1[1 + x % X1][10:26]
        grown[k * 16 : k * 16 + 16, :] = value if x < X1 else pltpu.roll(value, HALF, 1)
    grown[...] = exact(grown[...], spread)
    for i in range(16):
        value = grown[i * 16 : i * 16 + 12, :]
        twice[pl.ds(0, 12, stride=2), :] = value
        twice[pl.ds(1, 12, stride=2), :] = value
        first[1 + 2 * i] = corr[2 * i] + twice[...]
        first[2 + 2 * i] = corr[2 * i + 1] + twice[...]
    return fine


def turn_kernel(pos, b0, b1, b2, b3, b4, corr, resid, pairs, spread, merge, widen, after, lower, *scratch):
    strip, scratch = scratch[-1], scratch[:-1]
    tables = (spread[...], merge[...], widen[...])
    fine = coarse(pos, (b0, b1, b2, b3, b4), corr, resid, tables, scratch)
    first, second = scratch[-2:]
    sweep(fine, first, resid, second, 2, 3, 26)
    sweep(fine, second, resid, first, 4, 4, 24)
    sweep(fine, first, resid, second, 2, 5, 22)
    sweep(fine, second, resid, first, 4, 6, 20)
    for k in range(6, 26):
        after[k] = first[k + 1]
    for k in (0, 1, 2, 3, 4, 5, 26, 27, 28, 29, 30, 31):
        after[k] = jnp.zeros((YF, LANES), F32)
    lower_of(fine, first, resid, strip, pairs[...], lower)


def close_kernel(pos, b0, b1, b2, b3, b4, corr, resid, spread, merge, widen, start, out, *scratch):
    tables = (spread[...], merge[...], widen[...])
    fine = coarse(pos, (b0, b1, b2, b3, b4), corr, resid, tables, scratch)
    first, second = scratch[-2:]
    sweep(fine, first, resid, second, 2, 7, 18)
    sweep(fine, second, resid, first, 4, 8, 16)
    for k in range(16):
        out[k] = start[k] + first[9 + k][8:16]


def held(*shape):
    return pltpu.VMEM(shape, F32)


def shaped(*shape):
    return jax.ShapeDtypeStruct(shape, F32)


def inner():
    return [
        held(X1, Y1, LANES),
        held(X1 + 2, Y1, LANES),
        held(X1 + 2, Y1, LANES),
        held(X2, Y2, LANES),
        held(X2 + 2, Y2, LANES),
        held(X2 + 2, Y2, LANES),
        held(X2 * Y2, LANES),
        held(Y1, LANES),
        held(256, LANES),
        held(YF, LANES),
        held(XF + 2, YF, LANES),
        held(XF + 2, YF, LANES),
    ]


def many(body, name, count, shapes, scratch, limit=SMALL):
    return pl.pallas_call(
        body,
        name=name,
        in_specs=[SMEM] + [VMEM] * count,
        out_specs=[VMEM] * len(shapes),
        out_shape=shapes,
        scratch_shapes=scratch,
        compiler_params=pltpu.CompilerParams(vmem_limit_bytes=limit),
        interpret=INTERPRET,
    )


def opening(pos, near, fine, pairs, spread):
    shapes = [shaped(16, 8, LANES), shaped(XF, YF, LANES), shaped(XF, YF, LANES), shaped(16, LANES)]
    scratch = [held(XF + 2, YF, LANES)] * 3 + [held(256, LANES), held(YF, LANES), held(64, LANES)]
    return many(open_kernel, "opening", 4, shapes, scratch)(pos, near, fine, pairs, spread)


def turning(pos, blocks, corr, resid, tables):
    shapes = [shaped(XF, YF, LANES), shaped(16, LANES)]
    return many(turn_kernel, "turning", 11, shapes, inner() + [held(64, LANES)])(pos, *blocks, corr, resid, *tables)


def closing(pos, blocks, corr, resid, tables, start):
    return many(close_kernel, "closing", 11, [shaped(16, 8, LANES)], inner())(
        pos, *blocks, corr, resid, *tables[1:], start
    )[0]


def shifted(value, axes, size, step):
    return lax.ppermute(value, axes, [(i, i + step) for i in range(size) if 0 <= i + step < size])


def lay_kernel(*refs):
    parts, out, strip = refs[:9], refs[9], refs[10]
    for xx in range(4):
        for j in range(9):
            strip[4 * j : 4 * j + 4, :] = parts[j][4 * xx : 4 * xx + 4, :]
        out[xx] = strip[2:34, :]


def lay(parts):
    return pl.pallas_call(
        lay_kernel,
        name="lay",
        in_specs=[VMEM] * 9,
        out_specs=VMEM,
        out_shape=shaped(4, Y1, LANES),
        scratch_shapes=[held(40, LANES)],
        compiler_params=pltpu.CompilerParams(vmem_limit_bytes=SMALL),
        interpret=INTERPRET,
    )(*parts)


def gather(lower):
    sides = ("group", "gy")
    parts = [lower if step == 0 else shifted(lower, sides, YY, step) for step in (4, 3, 2, 1, 0, -1, -2, -3, -4)]
    block = lay([pltpu.with_memory_space_constraint(part, pltpu.VMEM) for part in parts])
    block = pltpu.with_memory_space_constraint(block, pltpu.VMEM)
    blocks = [block if step == 0 else shifted(block, "gx", GX, step) for step in (2, 1, 0, -1, -2)]
    return [pltpu.with_memory_space_constraint(block, pltpu.VMEM) for block in blocks]


def taller(fine):
    sides = ("group", "gy")
    return jnp.concatenate([shifted(fine, sides, YY, 1), fine, shifted(fine, sides, YY, -1)], axis=1)


def wider(tall):
    before = shifted(tall[8:16], "gx", GX, 1)
    behind = shifted(tall[0:8], "gx", GX, -1)
    return pltpu.with_memory_space_constraint(jnp.concatenate([before, tall, behind], axis=0), pltpu.VMEM)


def local(parent_mass, fine_mass, offsets):
    high, low, pairs, column, row, eigen = constants()
    spread = pairs.T
    spot = np.arange(LANES)
    merge = np.zeros((LANES, LANES), np.float32)
    merge[spot, spot % HALF // 2 + HALF * (spot // HALF)] = 1.0
    tables = (pairs, spread, jnp.asarray(merge, BF16), jnp.asarray(merge.T, BF16))
    pos = jnp.stack([lax.axis_index("gx"), lax.axis_index(("group", "gy"))]).astype(jnp.int32)
    wave = lax.dynamic_slice(eigen, (lax.axis_index(ALL),), (1,))
    tall = taller(fine_mass)
    got = swap(forward(offsets, parent_mass.reshape(NP, NP), fine_mass, high, low, pairs), FORE * LANES)
    got, tall = lax.optimization_barrier((got, tall))
    wide = wider(tall)
    got = swap(spectral(offsets, wave, got, high, low, column, row), BACK * LANES)
    near = near_back(offsets, got, high, low)
    start, resid, corr, lower = opening(pos, near, wide, pairs, spread)
    potential = whole_back(got, high, low)
    corr, lower = turning(pos, gather(lower), corr, resid, tables)
    out = closing(pos, gather(lower), corr, resid, tables, start)
    return (potential.reshape(WX, WY, NP), out)


def solution(mesh):
    spec = P("gx", ("group", "gy"), None)
    return jax.shard_map(
        local,
        mesh=mesh,
        in_specs=(spec, spec, P()),
        out_specs=(spec, spec),
        check_vma=False,
    )
```
